32 devices in a mesh: dp: 16 (over z, y, core), tensor: 2 (over x).
Axes of the slice: x: 2, y: 2, z: 4, core: 2. Of those that a mesh axis runs over, the one named last changes fastest.
Arguments:
- hidden_in: bfloat16 [8192, 1536], P('dp'), may hold values from -6 to 6
- norm_gain: float32 [1536], replicated, may hold values from 0.1 to 1.9
- weight_gate: bfloat16 [1536, 3072], P(None, 'tensor'), may hold values from -0.15625 to 0.15625
- weight_value: bfloat16 [1536, 3072], P(None, 'tensor'), may hold values from -0.15625 to 0.15625
- weight_step: bfloat16 [1536, 48], P(None, 'tensor'), may hold values from -0.15625 to 0.15625
- weight_scan: bfloat16 [1536, 256], replicated, may hold values from -0.15625 to 0.15625
- conv_value: float32 [4, 3072], P(None, 'tensor'), may hold values from -3 to 3
- conv_value_bias: float32 [3072], P('tensor'), may hold values from -0.5 to 0.5
- conv_scan: float32 [4, 256], replicated, may hold values from -3 to 3
- conv_scan_bias: float32 [256], replicated, may hold values from -0.5 to 0.5
- step_bias: float32 [48], P('tensor'), may hold values from -6.9 to -2.3
- decay_log: float32 [48], P('tensor'), may hold values from 0 to 2.77
- skip_gain: float32 [48], P('tensor'), may hold values from 0.5 to 1.5
- gate_gain: float32 [3072], P('tensor'), may hold values from 0.1 to 1.9
- weight_out: bfloat16 [3072, 1536], P('tensor'), may hold values from -0.15625 to 0.15625
- cotangent: bfloat16 [8192, 1536], P('dp'), may hold values from -6 to 6
Outputs:
- block_out: float32 [8192, 1536], P('dp', 'tensor')
- grad_in: float32 [8192, 1536], P('dp', 'tensor')
- grad_norm_gain: float32 [1536], P('tensor')
- grad_weight_gate: float32 [1536, 3072], P(None, 'tensor')
- grad_weight_value: float32 [1536, 3072], P(None, 'tensor')
- grad_weight_step: float32 [1536, 48], P(None, 'tensor')
- grad_weight_scan: float32 [1536, 256], replicated
- grad_conv_value: float32 [4, 3072], P(None, 'tensor')
- grad_conv_value_bias: float32 [3072], P('tensor')
- grad_conv_scan: float32 [4, 256], replicated
- grad_conv_scan_bias: float32 [256], replicated
- grad_step_bias: float32 [48], P('tensor')
- grad_decay_log: float32 [48], P('tensor')
- grad_skip: float32 [48], P('tensor')
- grad_gate_gain: float32 [3072], P('tensor')
- grad_weight_out: float32 [3072, 1536], P('tensor')
The draws below stay inside these ranges and needn't reach their ends.
All inputs are finite; a program needn't handle non-finite values.
Results may differ from the reference program's by a relative error of at most 0.0088.
Values sent between devices are 32-bit elements; how exact they have to be, the bound alone decides.
A program may use at most 192 MiB of HBM per device.

```python
import math
import jax
import jax.numpy as jnp
from jax import lax

D = 1536
HEADS = 48
STATE = 128
CONV = 4
SPAN = 256
SEQ_LEN = 512
INNER = 3072
SEQS = 16
TOKENS = 8192


def with_spikes(array, key, source, target, shards_of, factor):
    owner, partner = [(jnp.arange(array.shape[position]) // (array.shape[position] // shards_of)).reshape([-1 if axis == position else 1 for axis in range(array.ndim)]) for position in (source, target)]
    chosen = jax.random.permutation(key, shards_of)[partner]
    strong = (owner == chosen) | (owner == (partner + shards_of // 2) % shards_of)
    return jnp.where(strong, factor * array, array)


def level_of(stream_key, dims, cuts, least, largest):
    gain = 1.0
    for axis_at, shards_of in cuts:
        draws = jax.random.uniform(jax.random.fold_in(jax.random.fold_in(stream_key, 6), axis_at), (shards_of,), jnp.float32, least / len(cuts), largest / len(cuts))
        gain = gain * jnp.repeat(jnp.exp(draws), dims[axis_at] // shards_of).reshape((-1,) + (1,) * (len(dims) - 1 - axis_at))
    return gain


def scatter_about(rng, shape, spread, bound, split=(), kind=jnp.bfloat16):
    drawn = spread * jax.random.normal(rng, shape, jnp.float32)
    if split:
        drawn = drawn * level_of(rng, shape, split, -0.22, 0.18)
    return jnp.clip(drawn, -bound, bound).astype(kind)


def noise_with(rng, extent, scale, limit, cuts, heavy, kind=jnp.bfloat16):
    array = scale * jax.random.normal(rng, extent, jnp.float32)
    if cuts:
        array = array * level_of(rng, extent, cuts, -0.22, 0.18)
    return jnp.clip(with_spikes(array, jax.random.fold_in(rng, 3), *heavy), -limit, limit).astype(kind)


def setup_inputs(seed: int = 0) -> dict:
    streams_of = jax.random.split(jax.random.key(seed), 17)
    hidden_in = scatter_about(streams_of[0], (TOKENS, D), 1.0, 6.0, ((0, 16),))
    norm_gain = jnp.clip(1.0 + 0.18 * jax.random.normal(streams_of[1], (D,), jnp.float32), 0.1, 1.9)
    weight_gate = scatter_about(streams_of[2], (D, INNER), D ** -0.5, 0.15625, ((1, 2),))
    weight_value = scatter_about(streams_of[3], (D, INNER), D ** -0.5, 0.15625, ((1, 2),))
    weight_step = scatter_about(streams_of[4], (D, HEADS), D ** -0.5, 0.15625, ((1, 2),))
    weight_scan = scatter_about(streams_of[5], (D, 2 * STATE), D ** -0.5, 0.15625)
    conv_value = scatter_about(streams_of[6], (CONV, INNER), CONV ** -0.5, 3.0, ((1, 2),), jnp.float32)
    conv_value_bias = jnp.clip(jax.random.uniform(streams_of[7], (INNER,), jnp.float32, -0.5, 0.5) * level_of(streams_of[7], (INNER,), ((0, 2),), -0.4, 0.0), -0.5, 0.5)
    conv_scan = scatter_about(streams_of[8], (CONV, 2 * STATE), CONV ** -0.5, 3.0, (), jnp.float32)
    conv_scan_bias = jnp.clip(jax.random.uniform(streams_of[9], (2 * STATE,), jnp.float32, -0.5, 0.5), -0.5, 0.5)
    step_bias = jnp.clip(-6.9 + 4.6000001430511475 * jax.random.uniform(streams_of[10], (HEADS,), jnp.float32) ** level_of(streams_of[10], (HEADS,), ((0, 2),), -0.2, 0.2), -6.9, -2.3)
    decay_log = jnp.clip(2.77 * jax.random.uniform(streams_of[11], (HEADS,), jnp.float32) ** level_of(streams_of[11], (HEADS,), ((0, 2),), -0.2, 0.2), 0.0, 2.77)
    skip_gain = jnp.clip(0.5 + 1.0 * jax.random.uniform(streams_of[12], (HEADS,), jnp.float32) ** level_of(streams_of[12], (HEADS,), ((0, 2),), -0.2, 0.2), 0.5, 1.5)
    gate_gain = jnp.clip(1.0 + 0.18 * jax.random.normal(streams_of[13], (INNER,), jnp.float32), 0.1, 1.9)
    weight_out = noise_with(streams_of[14], (INNER, D), INNER ** -0.5, 0.15625, ((0, 2),), (0, 1, 2, 2.0))
    cotangent = scatter_about(streams_of[15], (TOKENS, D), 1.0, 6.0, ((0, 16),))
    return dict(hidden_in=hidden_in, norm_gain=norm_gain, weight_gate=weight_gate, weight_value=weight_value, weight_step=weight_step, weight_scan=weight_scan, conv_value=conv_value, conv_value_bias=conv_value_bias, conv_scan=conv_scan, conv_scan_bias=conv_scan_bias, step_bias=step_bias, decay_log=decay_log, skip_gain=skip_gain, gate_gain=gate_gain, weight_out=weight_out, cotangent=cotangent)


EPS = 1e-05
HIGHEST = lax.Precision.HIGHEST

def conv_silu(sequence, kernel, kernel_bias):
    kernel_width = kernel.shape[0]
    length = sequence.shape[1]
    padded = jnp.pad(sequence, ((0, 0), (kernel_width - 1, 0), (0, 0)))
    summed = jnp.zeros_like(sequence) + kernel_bias
    for offset in range(kernel_width):
        summed = summed + kernel[offset] * padded[:, offset:offset + length, :]
    return jax.nn.silu(summed)

def state_scan(head_input, step_size, rate, input_b, input_c, skip_gain):
    batch_size, length, head_count, head_width = head_input.shape
    block_count = length // SPAN
    state_dim = input_b.shape[-1]
    block_shape = (batch_size, block_count, SPAN)
    head_values = head_input.reshape(block_shape + (head_count, head_width))
    log_decay = (step_size * rate).reshape(block_shape + (head_count,))
    cumulative = jnp.cumsum(log_decay, axis=2)
    weighted = head_values * step_size.reshape(block_shape + (head_count,))[..., None]
    blocked_b = input_b.reshape(block_shape + (state_dim,))
    blocked_c = input_c.reshape(block_shape + (state_dim,))
    row_index = lax.broadcasted_iota(jnp.int32, (SPAN, SPAN), 0)
    col_index = lax.broadcasted_iota(jnp.int32, (SPAN, SPAN), 1)
    lower_mask = row_index >= col_index
    cum_heads = jnp.transpose(cumulative, (0, 1, 3, 2))
    decay_gaps = cum_heads[..., :, None] - cum_heads[..., None, :]
    decay_table = jnp.where(lower_mask, jnp.exp(jnp.where(lower_mask, decay_gaps, 0.0)), 0.0)
    intersection = jnp.einsum('bcin,bcjn->bcij', blocked_c, blocked_b, precision=HIGHEST)
    mix_table = decay_table * intersection[:, :, None]
    inner_part = jnp.einsum('bchij,bcjhp->bcihp', mix_table, weighted, precision=HIGHEST)
    span_total = cumulative[:, :, -1:, :]
    to_finish = jnp.exp(span_total - cumulative)
    span_states = jnp.einsum('bcjn,bcjhp->bchpn', blocked_b, weighted * to_finish[..., None], precision=HIGHEST)
    span_decay = jnp.exp(span_total[:, :, 0, :])

    def carry_step(carried, pieces):
        piece_state, piece_decay = pieces
        return (carried * piece_decay[..., None, None] + piece_state, carried)
    initial = jnp.zeros((batch_size, head_count, head_width, state_dim), jnp.float32)
    final_state, entering = lax.scan(carry_step, initial, (jnp.moveaxis(span_states, 1, 0), jnp.moveaxis(span_decay, 1, 0)))
    entering = jnp.moveaxis(entering, 0, 1)
    outer_part = jnp.einsum('bcin,bchpn->bcihp', blocked_c, entering, precision=HIGHEST) * jnp.exp(cumulative)[..., None]
    result = inner_part + outer_part + skip_gain[:, None] * head_values
    return result.reshape(batch_size, length, head_count * head_width)

def mixer_path(value_branch, scan_act, step_branch, conv_value, conv_value_bias, step_bias, decay_log, skip_gain):
    value_act = conv_silu(value_branch, conv_value, conv_value_bias)
    step_size = jax.nn.softplus(step_branch + step_bias)
    head_count = step_bias.shape[0]
    head_input = value_act.reshape(value_act.shape[:2] + (head_count, -1))
    half_width = scan_act.shape[-1] // 2
    return state_scan(head_input, step_size, -jnp.exp(decay_log), scan_act[..., :half_width], scan_act[..., half_width:], skip_gain)

def as_sequences(matrix, seq_count):
    return matrix.reshape(seq_count, -1, matrix.shape[-1])

def layer_pass(hidden, upstream, seq_count, params):
    norm_gain, weight_gate, weight_value, weight_step, weight_scan, conv_value, conv_value_bias, conv_scan, conv_scan_bias, step_bias, decay_log, skip_gain, gate_gain, weight_out = params
    tokens_here = hidden.shape[0]
    inputs = hidden.astype(jnp.float32)
    inv_rms = lax.rsqrt(lax.optimization_barrier(jnp.mean(inputs * inputs, axis=1)) + EPS)
    unit_in = inputs * inv_rms[:, None]
    normed = (unit_in * norm_gain).astype(jnp.bfloat16)
    gate_branch = jnp.dot(normed, weight_gate, preferred_element_type=jnp.float32)
    value_branch = jnp.dot(normed, weight_value, preferred_element_type=jnp.float32)
    step_branch = jnp.dot(normed, weight_step, preferred_element_type=jnp.float32)
    scan_branch = jnp.dot(normed, weight_scan, preferred_element_type=jnp.float32)
    scan_act, scan_pullback = jax.vjp(conv_silu, as_sequences(scan_branch, seq_count), conv_scan, conv_scan_bias)
    ssd_out, ssd_pullback = jax.vjp(mixer_path, as_sequences(value_branch, seq_count), scan_act, as_sequences(step_branch, seq_count), conv_value, conv_value_bias, step_bias, decay_log, skip_gain)
    ssd_flat = ssd_out.reshape(tokens_here, -1)
    gate_act = jax.nn.silu(gate_branch)
    gated = ssd_flat * gate_act
    inv_gate = lax.rsqrt(lax.optimization_barrier(jnp.mean(gated * gated, axis=1)) + EPS)
    unit_gate = gated * inv_gate[:, None]
    gate_normed = (unit_gate * gate_gain).astype(jnp.bfloat16)
    block_out = inputs + jnp.dot(gate_normed, weight_out, preferred_element_type=jnp.float32)
    d_normed = jnp.dot(upstream, weight_out.T, preferred_element_type=jnp.float32)
    grad_weight_out = jnp.dot(gate_normed.T, upstream, preferred_element_type=jnp.float32)
    grad_gate_gain = lax.optimization_barrier(jnp.sum(d_normed * unit_gate, axis=0))
    d_unit = d_normed * gate_gain
    d_gated = inv_gate[:, None] * (d_unit - unit_gate * lax.optimization_barrier(jnp.mean(d_unit * unit_gate, axis=1))[:, None])
    d_ssd = d_gated * gate_act
    sigmoid_gate = jax.nn.sigmoid(gate_branch)
    d_gate = d_gated * ssd_flat * sigmoid_gate * (1.0 + gate_branch * (1.0 - sigmoid_gate))
    d_value, d_scan_act, d_step, grad_conv_value, grad_conv_value_bias, grad_step_bias, grad_decay_log, grad_skip = ssd_pullback(d_ssd.reshape(ssd_out.shape))
    d_scan, grad_conv_scan, grad_conv_scan_bias = scan_pullback(d_scan_act)
    gate_rounded = d_gate.astype(jnp.bfloat16)
    value_rounded = d_value.reshape(tokens_here, -1).astype(jnp.bfloat16)
    step_rounded = d_step.reshape(tokens_here, -1).astype(jnp.bfloat16)
    scan_rounded = d_scan.reshape(tokens_here, -1).astype(jnp.bfloat16)
    grad_weight_gate = jnp.dot(normed.T, gate_rounded, preferred_element_type=jnp.float32)
    grad_weight_value = jnp.dot(normed.T, value_rounded, preferred_element_type=jnp.float32)
    grad_weight_step = jnp.dot(normed.T, step_rounded, preferred_element_type=jnp.float32)
    grad_weight_scan = jnp.dot(normed.T, scan_rounded, preferred_element_type=jnp.float32)
    d_normed_in = jnp.dot(gate_rounded, weight_gate.T, preferred_element_type=jnp.float32) + jnp.dot(value_rounded, weight_value.T, preferred_element_type=jnp.float32) + jnp.dot(step_rounded, weight_step.T, preferred_element_type=jnp.float32) + jnp.dot(scan_rounded, weight_scan.T, preferred_element_type=jnp.float32)
    grad_norm_gain = lax.optimization_barrier(jnp.sum(d_normed_in * unit_in, axis=0))
    d_unit_in = d_normed_in * norm_gain
    grad_in = upstream.astype(jnp.float32) + inv_rms[:, None] * (d_unit_in - unit_in * lax.optimization_barrier(jnp.mean(d_unit_in * unit_in, axis=1))[:, None])
    grads = (grad_norm_gain, grad_weight_gate, grad_weight_value, grad_weight_step, grad_weight_scan, grad_conv_value, grad_conv_value_bias, grad_conv_scan, grad_conv_scan_bias, grad_step_bias, grad_decay_log, grad_skip, grad_gate_gain, grad_weight_out)
    return (block_out, grad_in, grads)

def reference(hidden_in, norm_gain, weight_gate, weight_value, weight_step, weight_scan, conv_value, conv_value_bias, conv_scan, conv_scan_bias, step_bias, decay_log, skip_gain, gate_gain, weight_out, cotangent):
    params = (norm_gain, weight_gate, weight_value, weight_step, weight_scan, conv_value, conv_value_bias, conv_scan, conv_scan_bias, step_bias, decay_log, skip_gain, gate_gain, weight_out)
    group_size = math.gcd(SEQS, 4)
    block_tokens = group_size * SEQ_LEN
    block_count = SEQS // group_size

    def block_step(totals, block_index):
        first_row = (block_index * block_tokens).astype(jnp.int32)
        hidden = lax.dynamic_slice_in_dim(hidden_in, first_row, block_tokens, 0)
        upstream = lax.dynamic_slice_in_dim(cotangent, first_row, block_tokens, 0)
        block_out, grad_in, grads = layer_pass(hidden, upstream, group_size, params)
        return (tuple((previous + latest for previous, latest in zip(totals, grads))), (block_out, grad_in))
    initial = tuple((jnp.zeros(weight.shape, jnp.float32) for weight in params))
    totals, (outputs, grads_in) = lax.scan(block_step, initial, jnp.arange(block_count, dtype=jnp.int32))
    return (outputs.reshape(TOKENS, D), grads_in.reshape(TOKENS, D), totals[0], totals[1], totals[2], totals[3], totals[4], totals[5], totals[6], totals[7], totals[8], totals[9], totals[10], totals[11], totals[12], totals[13])
```

```python
import functools

import jax
import jax.numpy as jnp
from jax import lax
from jax.experimental import pallas as pl
from jax.experimental.pallas import tpu as pltpu
from jax.sharding import PartitionSpec as P

SPAN = 256
SEQ_LEN = 512
INNER = 3072

MESH = pl.DeviceIdType.MESH
GROUP = 32
TREES = 4


def grid_dims(dp_size):
    chips = dp_size // 2
    if chips == 8:
        return (4, 2)
    if chips == 32:
        return (2, 4, 4)
    return (chips,)


def build_trees(dims):
    count = 1
    for size in dims:
        count *= size

    def coords(node):
        out = []
        for size in reversed(dims):
            out.append(node % size)
            node //= size
        return tuple(reversed(out))

    def index(place):
        node = 0
        for size, at in zip(dims, place):
            node = node * size + at
        return node

    rank = len(dims)
    plans = []
    for tree in range(TREES):
        order = [(axis + 1 + tree // 2) % rank for axis in range(rank)]
        root = [
            (size - 1) // 2 if (tree % 2 == 0) else size // 2 for size in dims
        ]
        parent, children = [-1] * count, [[] for _ in range(count)]
        for node in range(count):
            place = list(coords(node))
            for axis in order:
                if place[axis] != root[axis]:
                    place[axis] += 1 if place[axis] < root[axis] else -1
                    parent[node] = index(place)
                    break
        for node in range(count):
            if parent[node] >= 0:
                children[parent[node]].append(node)

        def height(node):
            return max([0] + [1 + height(child) for child in children[node]])

        def depth(node):
            return 0 if parent[node] < 0 else 1 + depth(parent[node])

        plans.append(
            dict(
                parent=parent,
                children=children,
                slot=[
                    children[parent[node]].index(node) if parent[node] >= 0 else 0
                    for node in range(count)
                ],
                height=[height(node) for node in range(count)],
                depth=[depth(node) for node in range(count)],
                top=height(index(root)),
            )
        )
    return plans


def pick(me, table):
    value = jnp.int32(table[0])
    for at in range(1, len(table)):
        if table[at] != table[0] or True:
            value = jnp.where(me == at, jnp.int32(table[at]), value)
    return value


def all_reduce_kernel(
    plans, splits, hop, part, out, own_buf, sib_buf, up_buf, acc,
    own_sem, sib_send, sib_recv, up_send, up_recv, dn_send, dn_recv,
    tail_send, tail_recv, local_sem,
):
    depth_slots = own_buf.shape[0]
    width = own_buf.shape[2]
    rows = part.shape[0]
    chunks = rows // (2 * GROUP) * splits
    me = lax.axis_index("dp")
    core = lax.rem(me, 2)
    chip = me // 2
    sibling = me + 1 - 2 * core
    kids = up_buf.shape[1]
    first = 1
    node = []
    for plan in plans:
        parent = pick(chip, plan["parent"])
        node.append(
            dict(
                root=parent < 0,
                parent=parent * 2 + core,
                slot=pick(chip, plan["slot"]),
                kids=pick(chip, [len(c) for c in plan["children"]]),
                child=[
                    pick(chip, [c[i] if i < len(c) else 0 for c in plan["children"]]) * 2 + core
                    for i in range(kids)
                ],
                up=first + hop * pick(chip, plan["height"]),
                down=first + hop * (plan["top"] + pick(chip, plan["depth"])),
            )
        )
    last = first + hop * max(p["top"] + max(p["depth"]) for p in plans) + hop

    count = len(plans[0]["parent"])
    links = []
    for at in range(count):
        near = set()
        for plan in plans:
            if plan["parent"][at] >= 0:
                near.add(plan["parent"][at])
            near.update(plan["children"][at])
        links.append(sorted(near))
    most = max(len(near) for near in links)
    barrier = pltpu.get_barrier_semaphore()
    pl.semaphore_signal(barrier, inc=1, device_id={"dp": sibling}, device_id_type=MESH)
    degree = pick(chip, [len(near) for near in links])
    for at in range(most):
        other = pick(chip, [near[at] if at < len(near) else 0 for near in links]) * 2 + core

        @pl.when(at < degree)
        def _():
            pl.semaphore_signal(barrier, inc=1, device_id={"dp": other}, device_id_type=MESH)

    pl.semaphore_wait(barrier, degree + 1)

    def place(chunk, side, tree=None):
        row = (2 * (chunk // splits) + side) * GROUP
        height = GROUP
        if tree is not None:
            row = row + tree * (GROUP // TREES)
            height = GROUP // TREES
        col = lax.rem(chunk, splits) * width
        return pl.ds(pl.multiple_of(row, 8), height), pl.ds(pl.multiple_of(col, 128), width)

    def slot_of(chunk):
        return lax.rem(chunk, depth_slots)

    def own_copy(chunk):
        at = slot_of(chunk)
        return pltpu.make_async_copy(part.at[place(chunk, core)], own_buf.at[at], own_sem.at[at])

    def sib_copy(chunk):
        at = slot_of(chunk)
        return pltpu.make_async_remote_copy(
            part.at[place(chunk, 1 - core)], sib_buf.at[at], sib_send.at[at], sib_recv.at[at],
            device_id={"dp": sibling}, device_id_type=MESH,
        )

    def up_copy(tree, chunk):
        at = slot_of(chunk)
        return pltpu.make_async_remote_copy(
            acc.at[tree, at], up_buf.at[tree, node[tree]["slot"], at],
            up_send.at[tree, at], up_recv.at[tree, node[tree]["slot"], at],
            device_id={"dp": node[tree]["parent"]}, device_id_type=MESH,
        )

    def up_arrival(tree, kid, chunk):
        at = slot_of(chunk)
        return pltpu.make_async_remote_copy(
            acc.at[tree, at], up_buf.at[tree, kid, at],
            up_send.at[tree, at], up_recv.at[tree, kid, at],
            device_id={"dp": node[tree]["child"][kid]}, device_id_type=MESH,
        )

    def down_copy(tree, kid, chunk, at_root):
        at = slot_of(chunk)
        here = place(chunk, core, tree)
        return pltpu.make_async_remote_copy(
            acc.at[tree, at] if at_root else out.at[here], out.at[here],
            dn_send.at[tree, kid, at], dn_recv.at[tree, at],
            device_id={"dp": node[tree]["child"][kid]}, device_id_type=MESH,
        )

    def tail_copy(tree, chunk, at_root, side):
        at = slot_of(chunk)
        here = place(chunk, side, tree)
        return pltpu.make_async_remote_copy(
            acc.at[tree, at] if at_root else out.at[here], out.at[here],
            tail_send.at[tree, at], tail_recv.at[tree, at],
            device_id={"dp": sibling}, device_id_type=MESH,
        )

    def local_copy(tree, chunk):
        at = slot_of(chunk)
        return pltpu.make_async_copy(
            acc.at[tree, at], out.at[place(chunk, core, tree)], local_sem.at[tree, at]
        )

    def finish_sends(tree, chunk):
        info = node[tree]

        @pl.when(info["root"])
        def _():
            local_copy(tree, chunk).wait()

        @pl.when(jnp.logical_not(info["root"]))
        def _():
            up_copy(tree, chunk).wait_send()

        for kid in range(kids):
            @pl.when(kid < info["kids"])
            def _():
                down_copy(tree, kid, chunk, False).wait_send()

        tail_copy(tree, chunk, False, core).wait_send()

    def step(tick, _):
        for tree in range(TREES):
            chunk = tick - (node[tree]["down"] + hop)

            @pl.when((chunk >= 0) & (chunk < chunks))
            def _():
                tail_copy(tree, chunk, False, 1 - core).wait_recv()

        @pl.when(tick < chunks)
        def _():
            @pl.when(tick >= depth_slots)
            def _():
                sib_copy(tick - depth_slots).wait_send()

            own_copy(tick).start()
            sib_copy(tick).start()

        ready = tick - first

        @pl.when((ready >= 0) & (ready < chunks))
        def _():
            own_copy(ready).wait()
            sib_copy(ready).wait_recv()

        for tree in range(TREES):
            info = node[tree]
            chunk = tick - info["up"]
            rows_here = slice(tree * (GROUP // TREES), (tree + 1) * (GROUP // TREES))

            @pl.when((chunk >= 0) & (chunk < chunks))
            def _():
                at = slot_of(chunk)

                @pl.when(chunk >= depth_slots)
                def _():
                    finish_sends(tree, chunk - depth_slots)

                acc[tree, at] = own_buf[at, rows_here, :] + sib_buf[at, rows_here, :]
                for kid in range(kids):
                    @pl.when(kid < info["kids"])
                    def _():
                        up_arrival(tree, kid, chunk).wait_recv()
                        acc[tree, at] = acc[tree, at] + up_buf[tree, kid, at]

        for tree in range(TREES):
            info = node[tree]
            chunk = tick - info["up"]
            live = (chunk >= 0) & (chunk < chunks)

            @pl.when(live & jnp.logical_not(info["root"]))
            def _():
                up_copy(tree, chunk).start()

            @pl.when(live & info["root"])
            def _():
                for kid in range(kids):
                    @pl.when(kid < info["kids"])
                    def _():
                        down_copy(tree, kid, chunk, True).start()
                tail_copy(tree, chunk, True, core).start()
                local_copy(tree, chunk).start()

        for tree in range(TREES):
            info = node[tree]
            chunk = tick - info["down"]

            @pl.when((chunk >= 0) & (chunk < chunks) & jnp.logical_not(info["root"]))
            def _():
                down_copy(tree, 0, chunk, False).wait_recv()
                for kid in range(kids):
                    @pl.when(kid < info["kids"])
                    def _():
                        down_copy(tree, kid, chunk, False).start()
                tail_copy(tree, chunk, False, core).start()

        return 0

    lax.fori_loop(0, chunks + last, step, 0)

    def drain(at, _):
        chunk = chunks - depth_slots + at

        @pl.when(chunk >= 0)
        def _():
            sib_copy(chunk).wait_send()
            for tree in range(TREES):
                finish_sends(tree, chunk)

        return 0

    lax.fori_loop(0, depth_slots, drain, 0)


def tree_all_reduce(part, splits=1, hop=2):
    dp_size = lax.axis_size("dp")
    plans = build_trees(grid_dims(dp_size))
    kids = max(max(len(c) for c in p["children"]) for p in plans)
    reach = max(p["top"] + max(p["depth"]) for p in plans)
    slots = 1 + hop * (reach + 1) + 2
    rows, cols = part.shape
    width = cols // splits
    dma = pltpu.SemaphoreType.DMA
    small = GROUP // TREES
    return pl.pallas_call(
        functools.partial(all_reduce_kernel, plans, splits, hop),
        out_shape=jax.ShapeDtypeStruct((rows, cols), jnp.float32),
        in_specs=[pl.BlockSpec(memory_space=pl.ANY)],
        out_specs=pl.BlockSpec(memory_space=pl.ANY),
        scratch_shapes=[
            pltpu.VMEM((slots, GROUP, width), jnp.float32),
            pltpu.VMEM((slots, GROUP, width), jnp.float32),
            pltpu.VMEM((TREES, kids, slots, small, width), jnp.float32),
            pltpu.VMEM((TREES, slots, small, width), jnp.float32),
            dma((slots,)), dma((slots,)), dma((slots,)),
            dma((TREES, slots)), dma((TREES, kids, slots)),
            dma((TREES, kids, slots)), dma((TREES, slots)),
            dma((TREES, slots)), dma((TREES, slots)), dma((TREES, slots)),
        ],
        compiler_params=pltpu.CompilerParams(
            collective_id=0, has_side_effects=True, vmem_limit_bytes=60 << 20
        ),
    )(part)


EPS = 1e-05
HIGHEST = lax.Precision.HIGHEST


def conv_silu(sequence, kernel, kernel_bias):
    kernel_width = kernel.shape[0]
    length = sequence.shape[1]
    padded = jnp.pad(sequence, ((0, 0), (kernel_width - 1, 0), (0, 0)))
    summed = jnp.zeros_like(sequence) + kernel_bias
    for offset in range(kernel_width):
        summed = summed + kernel[offset] * padded[:, offset : offset + length, :]
    return jax.nn.silu(summed)


def state_scan(head_input, step_size, rate, input_b, input_c, skip_gain):
    batch_size, length, head_count, head_width = head_input.shape
    block_count = length // SPAN
    state_dim = input_b.shape[-1]
    block_shape = (batch_size, block_count, SPAN)
    head_values = head_input.reshape(block_shape + (head_count, head_width))
    log_decay = (step_size * rate).reshape(block_shape + (head_count,))
    cumulative = jnp.cumsum(log_decay, axis=2)
    weighted = head_values * step_size.reshape(block_shape + (head_count,))[..., None]
    blocked_b = input_b.reshape(block_shape + (state_dim,))
    blocked_c = input_c.reshape(block_shape + (state_dim,))
    row_index = lax.broadcasted_iota(jnp.int32, (SPAN, SPAN), 0)
    col_index = lax.broadcasted_iota(jnp.int32, (SPAN, SPAN), 1)
    lower_mask = row_index >= col_index
    cum_heads = jnp.transpose(cumulative, (0, 1, 3, 2))
    decay_gaps = cum_heads[..., :, None] - cum_heads[..., None, :]
    decay_table = jnp.where(lower_mask, jnp.exp(jnp.where(lower_mask, decay_gaps, 0.0)), 0.0)
    intersection = jnp.einsum("bcin,bcjn->bcij", blocked_c, blocked_b, precision=HIGHEST)
    mix_table = decay_table * intersection[:, :, None]
    inner_part = jnp.einsum("bchij,bcjhp->bcihp", mix_table, weighted, precision=HIGHEST)
    span_total = cumulative[:, :, -1:, :]
    to_finish = jnp.exp(span_total - cumulative)
    span_states = jnp.einsum(
        "bcjn,bcjhp->bchpn", blocked_b, weighted * to_finish[..., None], precision=HIGHEST
    )
    span_decay = jnp.exp(span_total[:, :, 0, :])

    def carry_step(carried, pieces):
        piece_state, piece_decay = pieces
        return (carried * piece_decay[..., None, None] + piece_state, carried)

    initial = jnp.zeros((batch_size, head_count, head_width, state_dim), jnp.float32)
    final_state, entering = lax.scan(
        carry_step, initial, (jnp.moveaxis(span_states, 1, 0), jnp.moveaxis(span_decay, 1, 0))
    )
    entering = jnp.moveaxis(entering, 0, 1)
    outer_part = (
        jnp.einsum("bcin,bchpn->bcihp", blocked_c, entering, precision=HIGHEST)
        * jnp.exp(cumulative)[..., None]
    )
    result = inner_part + outer_part + skip_gain[:, None] * head_values
    return result.reshape(batch_size, length, head_count * head_width)


def mixer_path(
    value_branch,
    scan_act,
    step_branch,
    conv_value,
    conv_value_bias,
    step_bias,
    decay_log,
    skip_gain,
):
    value_act = conv_silu(value_branch, conv_value, conv_value_bias)
    step_size = jax.nn.softplus(step_branch + step_bias)
    head_count = step_bias.shape[0]
    head_input = value_act.reshape(value_act.shape[:2] + (head_count, -1))
    half_width = scan_act.shape[-1] // 2
    return state_scan(
        head_input,
        step_size,
        -jnp.exp(decay_log),
        scan_act[..., :half_width],
        scan_act[..., half_width:],
        skip_gain,
    )


def as_sequences(matrix, seq_count):
    return matrix.reshape(seq_count, -1, matrix.shape[-1])


def per_device(
    hidden_in,
    norm_gain,
    weight_gate,
    weight_value,
    weight_step,
    weight_scan,
    conv_value,
    conv_value_bias,
    conv_scan,
    conv_scan_bias,
    step_bias,
    decay_log,
    skip_gain,
    gate_gain,
    weight_out,
    cotangent,
):
    tokens_here = hidden_in.shape[0]
    seq_count = tokens_here // SEQ_LEN
    model_width = hidden_in.shape[1]
    share_width = model_width // lax.axis_size("tensor")
    first_col = lax.axis_index("tensor") * share_width
    inputs = hidden_in.astype(jnp.float32)
    inv_rms = lax.rsqrt(jnp.mean(inputs * inputs, axis=1) + EPS)
    unit_in = inputs * inv_rms[:, None]
    normed = (unit_in * norm_gain).astype(jnp.bfloat16)
    gate_branch = jnp.dot(normed, weight_gate, preferred_element_type=jnp.float32)
    value_branch = jnp.dot(normed, weight_value, preferred_element_type=jnp.float32)
    step_branch = jnp.dot(normed, weight_step, preferred_element_type=jnp.float32)
    scan_branch = jnp.dot(normed, weight_scan, preferred_element_type=jnp.float32)
    scan_act, scan_pullback = jax.vjp(
        conv_silu, as_sequences(scan_branch, seq_count), conv_scan, conv_scan_bias
    )
    ssd_out, ssd_pullback = jax.vjp(
        mixer_path,
        as_sequences(value_branch, seq_count),
        scan_act,
        as_sequences(step_branch, seq_count),
        conv_value,
        conv_value_bias,
        step_bias,
        decay_log,
        skip_gain,
    )
    ssd_flat = ssd_out.reshape(tokens_here, -1)
    gate_act = jax.nn.silu(gate_branch)
    gated = ssd_flat * gate_act
    squares = lax.psum(jnp.sum(gated * gated, axis=1), "tensor")
    inv_gate = lax.rsqrt(squares / INNER + EPS)
    unit_gate = gated * inv_gate[:, None]
    gate_normed = (unit_gate * gate_gain).astype(jnp.bfloat16)
    partial_out = jnp.dot(gate_normed, weight_out, preferred_element_type=jnp.float32)
    summed_out = lax.psum(partial_out, "tensor")
    mixed_share = lax.dynamic_slice_in_dim(summed_out, first_col, share_width, 1)
    block_out = lax.dynamic_slice_in_dim(inputs, first_col, share_width, 1) + mixed_share
    d_normed = jnp.einsum("td,kd->tk", cotangent, weight_out, preferred_element_type=jnp.float32)
    grad_weight_out = jnp.einsum(
        "tk,td->kd", gate_normed, cotangent, preferred_element_type=jnp.float32
    )
    grad_gate_gain = jnp.sum(d_normed * unit_gate, axis=0)
    d_unit = d_normed * gate_gain
    gate_dot = lax.psum(jnp.sum(d_unit * unit_gate, axis=1), "tensor")
    d_gated = inv_gate[:, None] * (d_unit - unit_gate * (gate_dot / INNER)[:, None])
    d_ssd = d_gated * gate_act
    sigmoid_gate = jax.nn.sigmoid(gate_branch)
    d_gate = d_gated * ssd_flat * sigmoid_gate * (1.0 + gate_branch * (1.0 - sigmoid_gate))
    (
        d_value,
        d_scan_part,
        d_step,
        grad_conv_value,
        grad_conv_value_bias,
        grad_step_bias,
        grad_decay_log,
        grad_skip,
    ) = ssd_pullback(d_ssd.reshape(ssd_out.shape))
    d_scan_act = lax.psum(d_scan_part, "tensor")
    d_scan, grad_conv_scan, grad_conv_scan_bias = scan_pullback(d_scan_act)
    gate_rounded = d_gate.astype(jnp.bfloat16)
    value_rounded = d_value.reshape(tokens_here, -1).astype(jnp.bfloat16)
    step_rounded = d_step.reshape(tokens_here, -1).astype(jnp.bfloat16)
    scan_rounded = d_scan.reshape(tokens_here, -1).astype(jnp.bfloat16)
    grad_weight_gate = jnp.einsum(
        "td,tk->dk", normed, gate_rounded, preferred_element_type=jnp.float32
    )
    grad_weight_value = jnp.einsum(
        "td,tk->dk", normed, value_rounded, preferred_element_type=jnp.float32
    )
    grad_weight_step = jnp.einsum(
        "td,tk->dk", normed, step_rounded, preferred_element_type=jnp.float32
    )
    grad_weight_scan = jnp.einsum(
        "td,tk->dk", normed, scan_rounded, preferred_element_type=jnp.float32
    )
    partial_in = (
        jnp.einsum("tk,dk->td", gate_rounded, weight_gate, preferred_element_type=jnp.float32)
        + jnp.einsum("tk,dk->td", value_rounded, weight_value, preferred_element_type=jnp.float32)
        + jnp.einsum("tk,dk->td", step_rounded, weight_step, preferred_element_type=jnp.float32)
    )
    unit_share = lax.dynamic_slice_in_dim(unit_in, first_col, share_width, 1)
    gain_share = lax.dynamic_slice_in_dim(norm_gain, first_col, share_width, 0)
    d_normed_in = lax.psum(partial_in, "tensor") + jnp.einsum(
        "tk,dk->td", scan_rounded, weight_scan, preferred_element_type=jnp.float32
    )
    in_dot = jnp.sum(d_normed_in * norm_gain * unit_in, axis=1)
    d_share = lax.dynamic_slice_in_dim(d_normed_in, first_col, share_width, 1)
    d_unit_share = d_share * gain_share
    grad_norm_gain = jnp.sum(d_share * unit_share, axis=0)
    upstream_share = lax.dynamic_slice_in_dim(cotangent, first_col, share_width, 1).astype(
        jnp.float32
    )
    grad_in = upstream_share + inv_rms[:, None] * (
        d_unit_share - unit_share * (in_dot / model_width)[:, None]
    )
    wide = grad_weight_gate.shape[1]
    share = grad_norm_gain.shape[0]
    heads = grad_skip.shape[0]
    tail = jnp.concatenate(
        [grad_norm_gain, grad_step_bias, grad_decay_log, grad_skip, grad_conv_scan_bias]
    )
    small = jnp.concatenate(
        [
            grad_weight_step.T,
            grad_conv_value,
            grad_conv_value_bias[None],
            grad_gate_gain[None],
            jnp.pad(tail, (0, model_width - tail.shape[0]))[None],
            jnp.pad(grad_conv_scan.reshape(-1), (0, model_width - grad_conv_scan.size))[None],
        ]
    )
    scan_wide = grad_weight_scan.shape[1]
    rows = 3 * model_width + scan_wide + small.shape[0]
    spare = -rows % (2 * GROUP)
    packed = jnp.concatenate(
        [
            grad_weight_out,
            grad_weight_gate,
            grad_weight_value,
            grad_weight_scan.T,
            small,
            jnp.zeros((spare, model_width), jnp.float32),
        ]
    )
    summed = tree_all_reduce(packed)
    grad_weight_out = summed[:wide]
    grad_weight_gate = summed[wide : wide + model_width]
    grad_weight_value = summed[wide + model_width : wide + 2 * model_width]
    at = wide + 2 * model_width
    grad_weight_scan = summed[at : at + scan_wide].T
    at += scan_wide
    grad_weight_step = summed[at : at + heads].T
    at += heads
    grad_conv_value = summed[at : at + 4]
    grad_conv_value_bias = summed[at + 4]
    grad_gate_gain = summed[at + 5]
    line = summed[at + 6]
    grad_norm_gain = line[:share]
    grad_step_bias = line[share : share + heads]
    grad_decay_log = line[share + heads : share + 2 * heads]
    grad_skip = line[share + 2 * heads : share + 3 * heads]
    grad_conv_scan_bias = line[share + 3 * heads : share + 3 * heads + scan_wide]
    grad_conv_scan = summed[at + 7][: 4 * scan_wide].reshape(4, scan_wide)
    return (
        block_out,
        grad_in,
        grad_norm_gain,
        grad_weight_gate,
        grad_weight_value,
        grad_weight_step,
        grad_weight_scan,
        grad_conv_value,
        grad_conv_value_bias,
        grad_conv_scan,
        grad_conv_scan_bias,
        grad_step_bias,
        grad_decay_log,
        grad_skip,
        grad_gate_gain,
        grad_weight_out,
    )


def solution(mesh):
    placed = (
        P("dp", None),
        P(),
        P(None, "tensor"),
        P(None, "tensor"),
        P(None, "tensor"),
        P(),
        P(None, "tensor"),
        P("tensor"),
        P(),
        P(),
        P("tensor"),
        P("tensor"),
        P("tensor"),
        P("tensor"),
        P("tensor", None),
        P("dp", None),
    )
    return jax.shard_map(
        per_device,
        mesh=mesh,
        in_specs=placed,
        out_specs=(
            P("dp", "tensor"),
            P("dp", "tensor"),
            P("tensor"),
            P(None, "tensor"),
            P(None, "tensor"),
            P(None, "tensor"),
            P(),
            P(None, "tensor"),
            P("tensor"),
            P(),
            P(),
            P("tensor"),
            P("tensor"),
            P("tensor"),
            P("tensor"),
            P("tensor", None),
        ),
        check_vma=False,
    )
```
